128 devices in a mesh: aa: 4 (over x), ba: 4 (over z_hi, core), col: 8 (over y, z_lo).
Axes of the slice: x: 4, y: 4, z: 4 (z_hi: 2, z_lo: 2; z = z_hi * 2 + z_lo), core: 2. Of those that a mesh axis runs over, the one named last changes fastest.
Arguments:
- tokens: bfloat16 [64, 32, 64, 1024], P('aa', 'ba', 'col'), may hold values from -6 to 6
- norm_gain: float32 [1024], replicated, may hold values from 0.1 to 1.9
- in_weight: bfloat16 [1024, 3072], replicated, may hold values from -0.1875 to 0.1875
- skip_gain: float32 [1024], replicated, may hold values from 0.5 to 1.5
- spectrum_filter: bfloat16 [2, 64, 32, 64, 1024], P(None, ('ba', 'col'), None, None, 'aa'), may hold values from -4 to 4
- out_weight: bfloat16 [1024, 1024], replicated, may hold values from -0.1875 to 0.1875
Outputs:
- layer_out: bfloat16 [64, 32, 64, 1024], P('aa', 'ba', 'col')
The draws below stay inside these ranges and needn't reach their ends.
All inputs are finite; a program needn't handle non-finite values.
Results may differ from the reference program's by a relative error of at most 0.014.
Values may be sent and summed in bfloat16 or wider, within the bound.
A program may use at most 128 MiB of HBM per device.

```python
import math
import jax
import jax.numpy as jnp
from jax import lax

LA = 64
LB = 32
LC = 64
D = 1024


def steps_of(own_key, extent, split, smallest, largest):
    def one(dim, shards_of):
        heights = jax.random.uniform(jax.random.fold_in(jax.random.fold_in(own_key, 6), dim), (shards_of,), jnp.float32, smallest / len(split), largest / len(split))
        return jnp.repeat(jnp.exp(heights), extent[dim] // shards_of).reshape((-1,) + (1,) * (len(extent) - dim - 1))

    gain = one(*split[0])
    for cut in split[1:]:
        gain = gain * one(*cut)
    return gain


def centred(stream_key, shape, width, limit, pieces=(), kind=jnp.bfloat16):
    values = width * jax.random.normal(stream_key, shape, jnp.float32)
    if pieces:
        values = values * steps_of(stream_key, shape, pieces, -0.22, 0.18)
    return jnp.clip(values, -limit, limit).astype(kind)


def setup_inputs(seed: int = 0) -> dict:
    splits = jax.random.split(jax.random.key(seed), 7)
    return {
        "tokens": centred(splits[0], (LA, LB, LC, D), 1.0, 6.0, ((0, 4), (1, 4), (2, 8))),
        "norm_gain": jnp.clip(1.0 + 0.18 * jax.random.normal(splits[1], (D,), jnp.float32), 0.1, 1.9),
        "in_weight": centred(splits[2], (D, 3 * D), D ** -0.5, 0.1875),
        "skip_gain": jnp.clip(jax.random.uniform(splits[3], (D,), jnp.float32, 0.5, 1.5), 0.5, 1.5),
        "spectrum_filter": centred(splits[4], (2, LA, LB, LC, D), 0.7, 4.0, ((1, 32), (4, 4))),
        "out_weight": centred(splits[5], (D, D), D ** -0.5, 0.1875),
    }


EPSILON = 1e-06

def dft_tables(length):
    counter = jnp.arange(length, dtype=jnp.int32)
    product = counter[:, None] * counter[None, :] % length
    angle = 2.0 * math.pi / length * product.astype(jnp.float32)
    factor = 1.0 / math.sqrt(length)
    cos_table = (jnp.cos(angle) * factor).astype(jnp.bfloat16).astype(jnp.float32)
    sin_table = (jnp.sin(angle) * factor).astype(jnp.bfloat16).astype(jnp.float32)
    return (cos_table, sin_table)

def phase_pair(integer_phase, modulus):
    angle = 2.0 * math.pi / modulus * (integer_phase % modulus).astype(jnp.float32)
    return (jnp.cos(angle), jnp.sin(angle))

def rounded(value):
    return lax.optimization_barrier(value.astype(jnp.bfloat16)).astype(jnp.float32)

def reference(tokens, norm_gain, in_weight, skip_gain, spectrum_filter, out_weight):
    points = LA * LB * LC
    rows = tokens.reshape(LA, LB * LC, D)

    def project(block):
        flat = block.astype(jnp.float32)
        meansq = lax.optimization_barrier(jnp.mean(flat * flat, axis=-1, keepdims=True))
        normed = (flat * lax.rsqrt(meansq + EPSILON) * norm_gain).astype(jnp.bfloat16)
        projected = jnp.dot(normed, in_weight, preferred_element_type=jnp.float32)
        mixed_rows = (projected[:, :D] * projected[:, 2 * D:]).astype(jnp.bfloat16)
        gate_rows = projected[:, D:2 * D].astype(jnp.bfloat16)
        return (mixed_rows, gate_rows)
    mixed, gate = lax.map(project, rows)
    cos_a, sin_a = dft_tables(LA)
    cos_b, sin_b = dft_tables(LB)
    cos_c, sin_c = dft_tables(LC)
    freq_a = jnp.arange(LA, dtype=jnp.int32)
    index_j = jnp.arange(LB, dtype=jnp.int32)
    index_k = jnp.arange(LC, dtype=jnp.int32)
    cos_phi, sin_phi = phase_pair((LC * index_j[None, :, None] + index_k[None, None, :]) * freq_a[:, None, None], points)
    cos_phi = cos_phi[..., None]
    sin_phi = sin_phi[..., None]
    cos_psi, sin_psi = phase_pair(index_j[:, None] * index_k[None, :], LB * LC)
    cos_psi = cos_psi[None, :, :, None]
    sin_psi = sin_psi[None, :, :, None]
    group = 128 if D % 128 == 0 else D
    ngroups = D // group
    mixed_groups = mixed.reshape(LA, LB, LC, ngroups, group).transpose(3, 0, 1, 2, 4)
    filter_groups = spectrum_filter.reshape(2, LA, LB, LC, ngroups, group).transpose(4, 0, 1, 2, 3, 5)

    def spectral(operands):
        block, filt = operands
        source = block.astype(jnp.float32)
        real_part = jnp.einsum('fi,ijkc->fjkc', cos_a, source)
        imag_part = -jnp.einsum('fi,ijkc->fjkc', sin_a, source)
        first_real = rounded(real_part * cos_phi + imag_part * sin_phi)
        first_imag = rounded(imag_part * cos_phi - real_part * sin_phi)
        real_part = jnp.einsum('gj,fjkc->fgkc', cos_b, first_real) + jnp.einsum('gj,fjkc->fgkc', sin_b, first_imag)
        imag_part = jnp.einsum('gj,fjkc->fgkc', cos_b, first_imag) - jnp.einsum('gj,fjkc->fgkc', sin_b, first_real)
        second_real = rounded(real_part * cos_psi + imag_part * sin_psi)
        second_imag = rounded(imag_part * cos_psi - real_part * sin_psi)
        spec_real = jnp.einsum('hk,fgkc->fghc', cos_c, second_real) + jnp.einsum('hk,fgkc->fghc', sin_c, second_imag)
        spec_imag = jnp.einsum('hk,fgkc->fghc', cos_c, second_imag) - jnp.einsum('hk,fgkc->fghc', sin_c, second_real)
        filt_real = filt[0].astype(jnp.float32)
        filt_imag = filt[1].astype(jnp.float32)
        filtered_real = rounded(filt_real * spec_real - filt_imag * spec_imag)
        filtered_imag = rounded(filt_real * spec_imag + filt_imag * spec_real)
        real_part = jnp.einsum('hk,fghc->fgkc', cos_c, filtered_real) - jnp.einsum('hk,fghc->fgkc', sin_c, filtered_imag)
        imag_part = jnp.einsum('hk,fghc->fgkc', cos_c, filtered_imag) + jnp.einsum('hk,fghc->fgkc', sin_c, filtered_real)
        third_real = rounded(real_part * cos_psi - imag_part * sin_psi)
        third_imag = rounded(imag_part * cos_psi + real_part * sin_psi)
        real_part = jnp.einsum('gj,fgkc->fjkc', cos_b, third_real) - jnp.einsum('gj,fgkc->fjkc', sin_b, third_imag)
        imag_part = jnp.einsum('gj,fgkc->fjkc', cos_b, third_imag) + jnp.einsum('gj,fgkc->fjkc', sin_b, third_real)
        back_real = rounded(real_part * cos_phi - imag_part * sin_phi)
        back_imag = rounded(imag_part * cos_phi + real_part * sin_phi)
        result = jnp.einsum('fi,fjkc->ijkc', cos_a, back_real) - jnp.einsum('fi,fjkc->ijkc', sin_a, back_imag)
        return result.astype(jnp.bfloat16)
    conv_groups = lax.map(spectral, (mixed_groups, filter_groups))
    conv = conv_groups.transpose(1, 2, 3, 0, 4).reshape(LA, LB * LC, D)

    def finish(operands):
        conv_rows, gate_rows, mixed_rows = operands
        gated = (gate_rows.astype(jnp.float32) * (conv_rows.astype(jnp.float32) + skip_gain * mixed_rows.astype(jnp.float32))).astype(jnp.bfloat16)
        return jnp.dot(gated, out_weight, preferred_element_type=jnp.float32).astype(jnp.bfloat16)
    layer_out = lax.map(finish, (conv, gate, mixed))
    return layer_out.reshape(LA, LB, LC, D)
```

```python
import math

import jax
import jax.numpy as jnp
import numpy as np
from jax import lax
from jax.experimental import pallas as pl
from jax.experimental.pallas import tpu as pltpu
from jax.sharding import PartitionSpec as P

LA = 64
LB = 32
LC = 64
D = 1024
POINTS = LA * LB * LC
EPSILON = 1e-06
MESH = pl.DeviceIdType.MESH

NA, NB, NC = 4, 4, 8
SLOTS = NB * NC
NG = 4
NCC = 2
CHUNKS = NCC * NG
ROWS = 256
LANES = 128
HALF = LA // 2 + 1


def rounded(values):
    return np.asarray(values, np.float32).astype(jnp.bfloat16).astype(np.float32)


def dft_tables(length):
    counter = np.arange(length)
    angle = 2.0 * math.pi / length * (counter[:, None] * counter[None, :] % length)
    factor = 1.0 / math.sqrt(length)
    return rounded(np.cos(angle) * factor), rounded(np.sin(angle) * factor)


def static_tables():
    cos_a, sin_a = dft_tables(LA)
    small = np.zeros((HALF, 2, LA), np.float32)
    small[:, 0] = cos_a[:HALF]
    small[:, 1] = -sin_a[:HALF]
    small = small.reshape(HALF * 2, LA)
    table_a = np.repeat(small, 16, axis=1)
    table_lo = np.repeat(small[:LA].T, 16, axis=1)
    table_hi = np.repeat(small[2:].T, 16, axis=1)

    cos_b, sin_b = dft_tables(LB)
    lane = np.arange(512)
    j_of = 8 * (lane // 128) + 2 * (lane // 32 % 4) + lane // 8 % 2
    ri_of = lane // 16 % 2
    wc, ws = cos_b[:, j_of], sin_b[:, j_of]
    u2 = np.stack([np.where(ri_of, ws, wc), np.where(ri_of, wc, -ws)], 1).reshape(64, 512)
    v2 = np.stack([np.where(ri_of, wc, -ws), np.where(ri_of, -ws, -wc)], 1).reshape(64, 512)
    f0 = np.arange(LA)[:, None]
    sign = np.where((f0 >= LA // 2) & (ri_of[None] == 1), -1.0, 1.0)
    angle = 2.0 * math.pi / (LA * LB) * (f0 * j_of[None] % (LA * LB))
    cj, sj = np.cos(angle) * sign, np.sin(angle) * sign

    cos_c, sin_c = dft_tables(LC)
    lane = np.arange(128)
    k_of = 8 * (lane // 16) + lane % 8
    ri_of = lane // 8 % 2
    wc, ws = cos_c[:, k_of], sin_c[:, k_of]
    u3 = np.concatenate([np.where(ri_of, ws, wc), np.where(ri_of, wc, -ws)], 0)
    v3 = np.concatenate([np.where(ri_of, wc, -ws), np.where(ri_of, -ws, -wc)], 0)
    angle = 2.0 * math.pi / POINTS * (f0 * k_of[None] % POINTS)
    ca, sa = np.cos(angle), np.sin(angle)
    f1 = np.arange(LB)[:, None]
    angle = 2.0 * math.pi / (LB * LC) * (f1 * k_of[None] % (LB * LC))
    cb, sb = np.cos(angle), np.sin(angle)
    tables = (table_a, table_lo, table_hi, u2, v2, cj, sj, u3, v3, ca, sa, cb, sb)
    return tuple(np.asarray(t, np.float32) for t in tables)


def kernel(
    tok_hbm, gain_hbm, win_hbm, skip_hbm, filt_hbm, wout_hbm,
    ta_hbm, tlo_hbm, thi_hbm, u2_hbm, v2_hbm, cj_hbm, sj_hbm,
    u3_hbm, v3_hbm, ca_hbm, sa_hbm, cb_hbm, sb_hbm,
    out_hbm,
    tok, gain, wmix, wgate, skip, filt, wout,
    ta, tlo, thi, u2, v2, cj, sj, u3, v3, ca, sa, cb, sb,
    mixed, gate, xrecv, first, yzrecv, mid, mid2, bsend, brecv, csend, crecv, gated, outv,
    m1, mlo, mhi, t2, t2t, t3, t3t,
    lsem, osem, xs, xr, ys, yr, bs, br, cs, cr,
):
    a = lax.axis_index("aa")
    b = lax.axis_index("ba")
    c = lax.axis_index("col")
    s = b * NC + c

    loads = []

    def load(src, dst):
        copy = pltpu.make_async_copy(src, dst, lsem.at[len(loads)])
        copy.start()
        loads.append(copy)
        return copy

    first_loads = [load(gain_hbm, gain)]
    first_loads += [load(tok_hbm.at[:, pl.ds(16 * g, 16), :], tok.at[g]) for g in range(NG)]
    table_loads = [load(ta_hbm, ta), load(tlo_hbm, tlo), load(thi_hbm, thi)]
    mix_loads = []
    for cc in range(NCC):
        mix_loads.append([])
        for q in range(NA):
            for half, base in enumerate((0, 2 * D)):
                mix_loads[cc].append(
                    load(
                        win_hbm.at[:, pl.ds(base + 256 * q + 128 * cc, 128)],
                        wmix.at[cc, q, :, pl.ds(128 * half, 128)],
                    )
                )
    gate_loads = [load(win_hbm.at[:, pl.ds(D, D)], wgate)]
    late_loads = [
        load(src, dst)
        for src, dst in (
            (u2_hbm, u2), (v2_hbm, v2), (cj_hbm, cj), (sj_hbm, sj), (u3_hbm, u3), (v3_hbm, v3),
            (ca_hbm, ca), (sa_hbm, sa), (cb_hbm, cb), (sb_hbm, sb),
        )
    ]
    late_loads += [load(filt_hbm.at[..., pl.ds(128 * cc, 128)], filt.at[cc]) for cc in range(NCC)]
    end_loads = [load(skip_hbm, skip), load(wout_hbm, wout)]

    def x_device(d):
        return {"aa": lax.rem(a + d, NA), "ba": b, "col": c}

    def slot_of(d):
        return lax.rem(s + d, SLOTS)

    def yz_device(t):
        return {"aa": a, "ba": t // NC, "col": lax.rem(t, NC)}

    barrier = pltpu.get_barrier_semaphore()
    for d in range(1, NA):
        pl.semaphore_signal(barrier, inc=1, device_id=x_device(d), device_id_type=MESH)

    @pl.loop(1, SLOTS)
    def _(d):
        pl.semaphore_signal(barrier, inc=1, device_id=yz_device(slot_of(d)), device_id_type=MESH)

    for copy in table_loads:
        copy.wait()
    lane16 = lax.broadcasted_iota(jnp.int32, (16, 1024), 1)
    sub16 = lax.broadcasted_iota(jnp.int32, (16, 1024), 0)
    on16 = lax.rem(lane16, 16) == sub16

    @pl.loop(0, 2 * HALF)
    def _(r):
        m1[pl.ds(pl.multiple_of(16 * r, 16), 16), :] = jnp.where(on16, ta[pl.ds(r, 1), :], 0.0).astype(jnp.bfloat16)

    @pl.loop(0, LA)
    def _(r):
        at = pl.ds(pl.multiple_of(16 * r, 16), 16)
        mlo[at, :] = jnp.where(on16, tlo[pl.ds(r, 1), :], 0.0).astype(jnp.bfloat16)
        mhi[at, :] = jnp.where(on16, thi[pl.ds(r, 1), :], 0.0).astype(jnp.bfloat16)

    for copy in first_loads:
        copy.wait()

    @pl.loop(0, NG * 4)
    def _(n):
        g, part = n // 4, lax.rem(n, 4)
        view = tok.at[g, pl.ds(4 * part, 4)]
        block = view[...].astype(jnp.float32).reshape(64, D)
        scale = lax.rsqrt(jnp.mean(block * block, axis=-1, keepdims=True) + EPSILON)
        view[...] = (block * scale * gain[...]).astype(jnp.bfloat16).reshape(4, 16, D)

    pl.semaphore_wait(barrier, NA - 1 + SLOTS - 1)

    def x_copy(d, cc, g):
        to = lax.rem(a + d, NA)
        return pltpu.make_async_remote_copy(
            src_ref=mixed.at[to, cc, g], dst_ref=xrecv.at[cc, g, a],
            send_sem=xs.at[d, cc, g], recv_sem=xr.at[d, cc, g],
            device_id=x_device(d), device_id_type=MESH,
        )

    for cc in range(NCC):
        for copy in mix_loads[cc]:
            copy.wait()

        @pl.loop(0, NG)
        def _(g):
            rows = tok[g].reshape(ROWS, D)
            for q in range(NA):
                both = jnp.dot(rows, wmix[cc, q], preferred_element_type=jnp.float32)
                mixed[q, cc, g] = (both[:, :128] * both[:, 128:]).astype(jnp.bfloat16)
            for d in (2, 1, 3):
                x_copy(d, cc, g).start()
            xrecv[cc, g, a] = mixed[a, cc, g]

    def y_copy(d, cc, g):
        t = slot_of(d)
        p0 = jnp.where(t < SLOTS // 2, 2 * t, LA - 1 - 2 * t)
        return pltpu.make_async_remote_copy(
            src_ref=first.at[cc, g, pl.ds(p0, 2)], dst_ref=yzrecv.at[cc, :, c, b, g],
            send_sem=ys.at[d, cc, g], recv_sem=yr.at[d, cc, g],
            device_id=yz_device(t), device_id_type=MESH,
        )

    own0 = jnp.where(s < SLOTS // 2, 2 * s, LA - 1 - 2 * s)

    @pl.loop(0, CHUNKS)
    def _(n):
        cc, g = n // NG, lax.rem(n, NG)
        for d in (1, 3, 2):
            x_copy(d, cc, g).wait_recv()
        value = jnp.dot(m1[...], xrecv[cc, g].reshape(1024, LANES), preferred_element_type=jnp.float32)
        first[cc, g] = value.astype(jnp.bfloat16).reshape(HALF, 32, LANES)

        @pl.loop(1, SLOTS)
        def _(d):
            y_copy(d, cc, g).start()

        yzrecv[cc, :, c, b, g] = first[cc, g, pl.ds(own0, 2)]

    for copy in gate_loads:
        copy.wait()

    @pl.loop(0, NG)
    def _(g):
        value = jnp.dot(tok[g].reshape(ROWS, D), wgate[...], preferred_element_type=jnp.float32)
        gate[g] = value.astype(jnp.bfloat16)

    for copy in late_loads:
        copy.wait()
    lane8 = lax.broadcasted_iota(jnp.int32, (16, 512), 1)
    sub8 = lax.broadcasted_iota(jnp.int32, (16, 512), 0)
    on8 = lax.rem(lane8, 8) == lax.rem(sub8, 8)
    for u in range(2):
        f0 = jnp.where(s < SLOTS // 2, 2 * s + u, 2 * s + 1 - u)
        at0 = pl.ds(f0, 1)

        @pl.loop(0, LB)
        def _(f1):
            row0, row1 = pl.ds(2 * f1, 1), pl.ds(2 * f1 + 1, 1)
            up = u2[row0, :] * cj[at0, :] + v2[row0, :] * sj[at0, :]
            low = u2[row1, :] * cj[at0, :] + v2[row1, :] * sj[at0, :]
            value = jnp.where(on8, jnp.where(sub8 < 8, up, low), 0.0)
            t2[u, pl.ds(pl.multiple_of(16 * f1, 16), 16), :] = value.astype(jnp.bfloat16)

        @pl.loop(0, 4)
        def _(r):
            at = pl.ds(pl.multiple_of(128 * r, 128), 128)
            t2t[u, :, at] = jnp.transpose(t2[u, at, :].astype(jnp.float32)).astype(jnp.bfloat16)

        @pl.loop(0, LB)
        def _(f1):
            row = pl.ds(f1, 1)
            ec = ca[at0, :] * cb[row, :] - sa[at0, :] * sb[row, :]
            es = sa[at0, :] * cb[row, :] + ca[at0, :] * sb[row, :]
            value = u3[...] * ec + v3[...] * es
            t3[u, f1] = value.astype(jnp.bfloat16)
            t3t[u, f1] = jnp.transpose(value).astype(jnp.bfloat16)

    def b_copy(d, cc, g):
        t = slot_of(d)
        h = jnp.where(s < SLOTS // 2, 0, 1)
        q = jnp.where(s < SLOTS // 2, s, SLOTS - 1 - s)
        return pltpu.make_async_remote_copy(
            src_ref=bsend.at[cc, :, lax.rem(t, NC), t // NC, g], dst_ref=brecv.at[cc, g, h, q],
            send_sem=bs.at[d, cc, g], recv_sem=br.at[d, cc, g],
            device_id=yz_device(t), device_id_type=MESH,
        )

    own_h = jnp.where(s < SLOTS // 2, 0, 1)
    own_q = jnp.where(s < SLOTS // 2, s, SLOTS - 1 - s)

    @pl.loop(0, NCC)
    def _(cc):
        @pl.loop(1, SLOTS)
        def _(d):
            for g in range(NG):
                y_copy(d, cc, g).wait_recv()

        @pl.loop(0, 2)
        def _(u):
            l = jnp.where(s < SLOTS // 2, u, 1 - u)

            @pl.loop(0, NC // 2)
            def _(n):
                pair = [yzrecv[cc, u, 2 * n + m].reshape(512, LANES) for m in range(2)]
                value = jnp.dot(t2[u], jnp.concatenate(pair, axis=1), preferred_element_type=jnp.float32)
                value = value.astype(jnp.bfloat16)
                for m in range(2):
                    mid[:, 2 * n + m] = value[:, 128 * m : 128 * (m + 1)].reshape(LB, 16, LANES)

            @pl.loop(0, LB // 4)
            def _(n):
                spectra = []
                for e in range(4):
                    f1 = 4 * n + e
                    spectra.append(
                        jnp.dot(t3[u, f1], mid[f1].reshape(128, LANES), preferred_element_type=jnp.float32)
                    )
                outs = []
                for e in range(4):
                    f1 = 4 * n + e
                    xr_, xi_ = spectra[e][:64], spectra[e][64:]
                    hr = filt[cc, 0, l, f1].astype(jnp.float32)
                    hi = filt[cc, 1, l, f1].astype(jnp.float32)
                    outs.append(
                        jnp.concatenate([hr * xr_ - hi * xi_, hr * xi_ + hi * xr_], axis=0).astype(jnp.bfloat16)
                    )
                for e in range(4):
                    f1 = 4 * n + e
                    value = jnp.dot(t3t[u, f1], outs[e], preferred_element_type=jnp.float32)
                    mid2[f1] = value.astype(jnp.bfloat16).reshape(NC, 16, LANES)

            @pl.loop(0, NC // 2)
            def _(n):
                pair = [mid2[:, 2 * n + m].reshape(512, LANES) for m in range(2)]
                value = jnp.dot(t2t[u], jnp.concatenate(pair, axis=1), preferred_element_type=jnp.float32)
                value = value.astype(jnp.bfloat16)
                for m in range(2):
                    bsend[cc, u, 2 * n + m] = value[:, 128 * m : 128 * (m + 1)].reshape(NB, NG, 32, LANES)

        @pl.loop(0, NG)
        def _(g):
            @pl.loop(1, SLOTS)
            def _(d):
                b_copy(d, cc, g).start()

            brecv[cc, g, own_h, own_q] = bsend[cc, :, c, b, g]

    def c_copy(d, cc, g):
        to = lax.rem(a + d, NA)
        return pltpu.make_async_remote_copy(
            src_ref=csend.at[cc, g, to], dst_ref=crecv.at[cc, g, a],
            send_sem=cs.at[d, cc, g], recv_sem=cr.at[d, cc, g],
            device_id=x_device(d), device_id_type=MESH,
        )

    for copy in end_loads:
        copy.wait()

    @pl.loop(0, CHUNKS)
    def _(n):
        cc, g = n // NG, lax.rem(n, NG)

        @pl.loop(1, SLOTS)
        def _(d):
            b_copy(d, cc, g).wait_recv()

        value = jnp.dot(mlo[...], brecv[cc, g, 0].reshape(1024, LANES), preferred_element_type=jnp.float32)
        value += jnp.dot(mhi[...], brecv[cc, g, 1].reshape(1024, LANES), preferred_element_type=jnp.float32)
        csend[cc, g] = value.astype(jnp.bfloat16).reshape(NA, ROWS, LANES)
        for d in (2, 1, 3):
            c_copy(d, cc, g).start()
        crecv[cc, g, a] = csend[cc, g, a]

    def out_copy(g):
        return pltpu.make_async_copy(outv.at[g], out_hbm.at[:, pl.ds(16 * g, 16), :], osem.at[g])

    for g in range(NG):
        for cc in range(NCC):
            for d in (1, 3, 2):
                c_copy(d, cc, g).wait_recv()
        for q in range(NA):
            for cc in range(NCC):
                at = pl.ds(256 * q + 128 * cc, 128)
                conv = crecv[cc, g, q].astype(jnp.float32)
                plus = conv + skip[:, at] * mixed[q, cc, g].astype(jnp.float32)
                gated[:, at] = (gate[g, :, at].astype(jnp.float32) * plus).astype(jnp.bfloat16)
        value = jnp.dot(gated[...], wout[...], preferred_element_type=jnp.float32)
        outv[g] = value.astype(jnp.bfloat16).reshape(16, 16, D)
        out_copy(g).start()

    @pl.loop(0, CHUNKS)
    def _(n):
        cc, g = n // NG, lax.rem(n, NG)
        for d in range(1, NA):
            x_copy(d, cc, g).wait_send()
            c_copy(d, cc, g).wait_send()

        @pl.loop(1, SLOTS)
        def _(d):
            y_copy(d, cc, g).wait_send()
            b_copy(d, cc, g).wait_send()

    for g in range(NG):
        out_copy(g).wait()


def local(tokens, norm_gain, in_weight, skip_gain, spectrum_filter, out_weight):
    tables = [jnp.asarray(t) for t in static_tables()]
    bf, f32 = jnp.bfloat16, jnp.float32
    vmem = pltpu.VMEM
    dma = pltpu.SemaphoreType.DMA
    scratch = [
        vmem((NG, 16, 16, D), bf), vmem((1, D), f32), vmem((NCC, NA, D, 256), bf), vmem((D, D), bf),
        vmem((1, D), f32), vmem((NCC, 2, 2, LB, LC, LANES), bf), vmem((D, D), bf),
        *[vmem(t.shape, f32) for t in tables],
        vmem((NA, NCC, NG, ROWS, LANES), bf),
        vmem((NG, ROWS, D), bf),
        vmem((NCC, NG, NA, ROWS, LANES), bf),
        vmem((NCC, NG, HALF, 32, LANES), bf),
        vmem((NCC, 2, NC, NB, NG, 32, LANES), bf),
        vmem((LB, NC, 16, LANES), bf),
        vmem((LB, NC, 16, LANES), bf),
        vmem((NCC, 2, NC, NB, NG, 32, LANES), bf),
        vmem((NCC, NG, 2, 16, 2, 32, LANES), bf),
        vmem((NCC, NG, NA, ROWS, LANES), bf),
        vmem((NCC, NG, NA, ROWS, LANES), bf),
        vmem((ROWS, D), bf),
        vmem((NG, 16, 16, D), bf),
        vmem((HALF * 32, 1024), bf), vmem((1024, 1024), bf), vmem((1024, 1024), bf),
        vmem((2, 512, 512), bf), vmem((2, 512, 512), bf),
        vmem((2, LB, 128, 128), bf), vmem((2, LB, 128, 128), bf),
        dma((40,)), dma((NG,)),
        dma((NA, NCC, NG)), dma((NA, NCC, NG)),
        dma((SLOTS, NCC, NG)), dma((SLOTS, NCC, NG)),
        dma((SLOTS, NCC, NG)), dma((SLOTS, NCC, NG)),
        dma((NA, NCC, NG)), dma((NA, NCC, NG)),
    ]
    out = pl.pallas_call(
        kernel,
        out_shape=jax.ShapeDtypeStruct((16, 64, D), bf),
        in_specs=[pl.BlockSpec(memory_space=pl.ANY)] * (6 + len(tables)),
        out_specs=pl.BlockSpec(memory_space=pl.ANY),
        scratch_shapes=scratch,
        compiler_params=pltpu.CompilerParams(
            collective_id=0, has_side_effects=True, vmem_limit_bytes=67043328
        ),
    )(
        tokens.reshape(16, 64, D), norm_gain.reshape(1, D), in_weight, skip_gain.reshape(1, D),
        spectrum_filter, out_weight, *tables,
    )
    return out.reshape(16, 8, 8, D)


def solution(mesh):
    in_specs = (
        P("aa", "ba", "col", None),
        P(),
        P(),
        P(),
        P(None, ("ba", "col"), None, None, "aa"),
        P(),
    )
    out_specs = P("aa", "ba", "col", None)
    return jax.shard_map(local, mesh=mesh, in_specs=in_specs, out_specs=out_specs, check_vma=False)
```

```python
import math

import jax
import jax.numpy as jnp
import numpy as np
from jax import lax
from jax.experimental import pallas as pl
from jax.experimental.pallas import tpu as pltpu
from jax.sharding import PartitionSpec as P

LA = 64
LB = 32
LC = 64
D = 1024
POINTS = LA * LB * LC
EPSILON = 1e-06
MESH = pl.DeviceIdType.MESH

NA, NB, NC = 4, 4, 8
SLOTS = NB * NC
NG = 4
NCC = 2
CHUNKS = NCC * NG
ROWS = 256
LANES = 128
HALF = LA // 2 + 1


def rounded(values):
    return np.asarray(values, np.float32).astype(jnp.bfloat16).astype(np.float32)


def dft_tables(length):
    counter = np.arange(length)
    angle = 2.0 * math.pi / length * (counter[:, None] * counter[None, :] % length)
    factor = 1.0 / math.sqrt(length)
    return rounded(np.cos(angle) * factor), rounded(np.sin(angle) * factor)


def static_tables():
    cos_a, sin_a = dft_tables(LA)
    small = np.zeros((HALF, 2, LA), np.float32)
    small[:, 0] = cos_a[:HALF]
    small[:, 1] = -sin_a[:HALF]
    small = small.reshape(HALF * 2, LA)
    table_a = np.repeat(small, 16, axis=1)
    table_lo = np.repeat(small[:LA].T, 16, axis=1)
    table_hi = np.repeat(small[2:].T, 16, axis=1)

    cos_b, sin_b = dft_tables(LB)
    lane = np.arange(512)
    j_of = 8 * (lane // 128) + 2 * (lane // 32 % 4) + lane // 8 % 2
    ri_of = lane // 16 % 2
    wc, ws = cos_b[:, j_of], sin_b[:, j_of]
    u2 = np.stack([np.where(ri_of, ws, wc), np.where(ri_of, wc, -ws)], 1).reshape(64, 512)
    v2 = np.stack([np.where(ri_of, wc, -ws), np.where(ri_of, -ws, -wc)], 1).reshape(64, 512)
    f0 = np.arange(LA)[:, None]
    sign = np.where((f0 >= LA // 2) & (ri_of[None] == 1), -1.0, 1.0)
    angle = 2.0 * math.pi / (LA * LB) * (f0 * j_of[None] % (LA * LB))
    cj, sj = np.cos(angle) * sign, np.sin(angle) * sign

    cos_c, sin_c = dft_tables(LC)
    lane = np.arange(128)
    k_of = 8 * (lane // 16) + lane % 8
    ri_of = lane // 8 % 2
    wc, ws = cos_c[:, k_of], sin_c[:, k_of]
    u3 = np.concatenate([np.where(ri_of, ws, wc), np.where(ri_of, wc, -ws)], 0)
    v3 = np.concatenate([np.where(ri_of, wc, -ws), np.where(ri_of, -ws, -wc)], 0)
    angle = 2.0 * math.pi / POINTS * (f0 * k_of[None] % POINTS)
    ca, sa = np.cos(angle), np.sin(angle)
    f1 = np.arange(LB)[:, None]
    angle = 2.0 * math.pi / (LB * LC) * (f1 * k_of[None] % (LB * LC))
    cb, sb = np.cos(angle), np.sin(angle)
    tables = (
        table_a, np.stack([table_lo, table_hi]), np.stack([u2, v2, cj, sj]),
        np.stack([u3, v3]), np.stack([ca, sa]), np.stack([cb, sb]),
    )
    return tuple(np.asarray(t, np.float32) for t in tables)


def kernel(
    tok_hbm, gain_hbm, win_hbm, skip_hbm, filt_hbm, wout_hbm,
    ta_hbm, tinv_hbm, two_hbm, three_hbm, tca_hbm, tcb_hbm,
    outv,
    tok, gain, wmix, wgate, skip, filt, wout,
    ta, tinv, two, three, tca, tcb,
    mixed, gate, xrecv, first, yzrecv, mid, mid2, bsend, brecv, csend, crecv, gated,
    m1, mlo, mhi, t2, t2t, t3, t3t,
    lsem, ss, xr, yr, br, cr,
):
    a = lax.axis_index("aa")
    b = lax.axis_index("ba")
    c = lax.axis_index("col")
    s = b * NC + c

    def fetch(n, src, dst):
        pltpu.make_async_copy(src, dst, lsem.at[n]).start()

    def landed(sem, ref):
        pltpu.make_async_copy(ref, ref, sem).wait()

    fetch(0, gain_hbm, gain)
    for g in range(NG):
        fetch(1 + g, tok_hbm.at[:, pl.ds(16 * g, 16), :], tok.at[g])
    for cc in range(NCC):
        for q in range(NA):
            for half, base in enumerate((0, 2 * D)):
                fetch(
                    5 + cc,
                    win_hbm.at[:, pl.ds(base + 256 * q + 128 * cc, 128)],
                    wmix.at[cc, q, :, pl.ds(128 * half, 128)],
                )
    fetch(7, ta_hbm, ta)
    fetch(8, tinv_hbm, tinv)
    fetch(9, win_hbm.at[:, pl.ds(D, D)], wgate)
    fetch(10, two_hbm, two)
    fetch(11, three_hbm, three)
    fetch(12, tca_hbm, tca)
    fetch(13, tcb_hbm, tcb)
    for cc in range(NCC):
        fetch(14 + cc, filt_hbm.at[..., pl.ds(128 * cc, 128)], filt.at[cc])
    fetch(16, skip_hbm, skip)
    fetch(17, wout_hbm, wout)

    def x_device(d):
        return {"aa": lax.rem(a + d, NA), "ba": b, "col": c}

    bits = [lax.rem(c, 2), lax.rem(c // 2, 2), c // 4, lax.rem(b, 2), b // 2]

    def partner(d):
        picked = [1 - bit if d >> n & 1 else bit for n, bit in enumerate(bits)]
        return picked[3] + 2 * picked[4], picked[0] + 2 * picked[1] + 4 * picked[2]

    def yz_device(tb, tc):
        return {"aa": a, "ba": tb, "col": tc}

    barrier = pltpu.get_barrier_semaphore()
    for d in range(1, NA):
        pl.semaphore_signal(barrier, inc=1, device_id=x_device(d), device_id_type=MESH)

    for d in range(1, SLOTS):
        pl.semaphore_signal(barrier, inc=1, device_id=yz_device(*partner(d)), device_id_type=MESH)

    def x_copy(d, cc, g):
        to = lax.rem(a + d, NA)
        return pltpu.make_async_remote_copy(
            src_ref=mixed.at[to, cc, g], dst_ref=xrecv.at[cc, g, a],
            send_sem=ss.at[0], recv_sem=xr.at[cc, g],
            device_id=x_device(d), device_id_type=MESH,
        )

    def mix(cc, g):
        rows = tok[g].reshape(ROWS, D)
        for q in range(NA):
            both = jnp.dot(rows, wmix[cc, q], preferred_element_type=jnp.float32)
            mixed[q, cc, g] = (both[:, :128] * both[:, 128:]).astype(jnp.bfloat16)

    def mix_send(cc, g):
        for d in (2, 1, 3):
            x_copy(d, cc, g).start()
        xrecv[cc, g, a] = mixed[a, cc, g]

    landed(lsem.at[0], gain)
    for g in range(NG):
        landed(lsem.at[1 + g], tok.at[g])

        @pl.loop(0, 4)
        def _(part):
            view = tok.at[g, pl.ds(4 * part, 4)]
            block = view[...].astype(jnp.float32).reshape(64, D)
            scale = lax.rsqrt(jnp.mean(block * block, axis=-1, keepdims=True) + EPSILON)
            view[...] = (block * scale * gain[...]).astype(jnp.bfloat16).reshape(4, 16, D)

        if g == 0:
            landed(lsem.at[5], wmix.at[0])
        mix(0, g)
        if g == 0:
            pl.semaphore_wait(barrier, NA - 1 + SLOTS - 1)
        mix_send(0, g)

    landed(lsem.at[7], ta)
    lane16 = lax.broadcasted_iota(jnp.int32, (16, 1024), 1)
    sub16 = lax.broadcasted_iota(jnp.int32, (16, 1024), 0)
    on16 = lax.rem(lane16, 16) == sub16

    @pl.loop(0, 2 * HALF)
    def _(r):
        m1[pl.ds(pl.multiple_of(16 * r, 16), 16), :] = jnp.where(on16, ta[pl.ds(r, 1), :], 0.0).astype(jnp.bfloat16)

    landed(lsem.at[6], wmix.at[1])

    def y_copy(d, cc, g):
        tb, tc = partner(d)
        t = tb * NC + tc
        p0 = jnp.where(t < SLOTS // 2, 2 * t, LA - 1 - 2 * t)
        return pltpu.make_async_remote_copy(
            src_ref=first.at[cc, g, pl.ds(p0, 2)], dst_ref=yzrecv.at[cc, :, c, b, g],
            send_sem=ss.at[1], recv_sem=yr.at[cc, g],
            device_id=yz_device(tb, tc), device_id_type=MESH,
        )

    own0 = jnp.where(s < SLOTS // 2, 2 * s, LA - 1 - 2 * s)

    @pl.loop(0, CHUNKS)
    def _(n):
        cc, g = n // NG, lax.rem(n, NG)
        landed(xr.at[cc, g], xrecv.at[cc, g, pl.ds(0, NA - 1)])
        value = jnp.dot(m1[...], xrecv[cc, g].reshape(1024, LANES), preferred_element_type=jnp.float32)
        first[cc, g] = value.astype(jnp.bfloat16).reshape(HALF, 32, LANES)

        for d in range(1, SLOTS):
            y_copy(d, cc, g).start()

        yzrecv[cc, :, c, b, g] = first[cc, g, pl.ds(own0, 2)]

        @pl.when(n < NG)
        def _():
            mix(1, n)
            mix_send(1, n)

    landed(lsem.at[9], wgate)

    @pl.loop(0, NG)
    def _(g):
        value = jnp.dot(tok[g].reshape(ROWS, D), wgate[...], preferred_element_type=jnp.float32)
        gate[g] = value.astype(jnp.bfloat16)

    landed(lsem.at[10], two)
    landed(lsem.at[11], three)
    landed(lsem.at[12], tca)
    landed(lsem.at[13], tcb)
    for cc in range(NCC):
        landed(lsem.at[14 + cc], filt.at[cc])
    landed(lsem.at[8], tinv)

    @pl.loop(0, LA)
    def _(r):
        at = pl.ds(pl.multiple_of(16 * r, 16), 16)
        mlo[at, :] = jnp.where(on16, tinv[0, pl.ds(r, 1), :], 0.0).astype(jnp.bfloat16)
        mhi[at, :] = jnp.where(on16, tinv[1, pl.ds(r, 1), :], 0.0).astype(jnp.bfloat16)

    lane8 = lax.broadcasted_iota(jnp.int32, (16, 512), 1)
    sub8 = lax.broadcasted_iota(jnp.int32, (16, 512), 0)
    on8 = lax.rem(lane8, 8) == lax.rem(sub8, 8)
    for u in range(2):
        f0 = jnp.where(s < SLOTS // 2, 2 * s + u, 2 * s + 1 - u)
        at0 = pl.ds(f0, 1)

        @pl.loop(0, LB)
        def _(f1):
            row0, row1 = pl.ds(2 * f1, 1), pl.ds(2 * f1 + 1, 1)
            up = two[0, row0, :] * two[2, at0, :] + two[1, row0, :] * two[3, at0, :]
            low = two[0, row1, :] * two[2, at0, :] + two[1, row1, :] * two[3, at0, :]
            value = jnp.where(on8, jnp.where(sub8 < 8, up, low), 0.0)
            t2[u, pl.ds(pl.multiple_of(16 * f1, 16), 16), :] = value.astype(jnp.bfloat16)

        @pl.loop(0, 4)
        def _(r):
            at = pl.ds(pl.multiple_of(128 * r, 128), 128)
            t2t[u, :, at] = jnp.transpose(t2[u, at, :].astype(jnp.float32)).astype(jnp.bfloat16)

        @pl.loop(0, LB)
        def _(f1):
            row = pl.ds(f1, 1)
            ec = tca[0, at0, :] * tcb[0, row, :] - tca[1, at0, :] * tcb[1, row, :]
            es = tca[1, at0, :] * tcb[0, row, :] + tca[0, at0, :] * tcb[1, row, :]
            value = three[0] * ec + three[1] * es
            t3[u, f1] = value.astype(jnp.bfloat16)
            t3t[u, f1] = jnp.transpose(value).astype(jnp.bfloat16)

    place = jnp.where(s < SLOTS // 2, 2 * s, 32 + 2 * (SLOTS - 1 - s))

    def b_copy(d, cc, g):
        tb, tc = partner(d)
        return pltpu.make_async_remote_copy(
            src_ref=bsend.at[cc, :, tc, tb, g], dst_ref=brecv.at[cc, g, pl.ds(place, 2)],
            send_sem=ss.at[2], recv_sem=br.at[cc, g],
            device_id=yz_device(tb, tc), device_id_type=MESH,
        )


    @pl.loop(0, NCC)
    def _(cc):
        for g in range(NG):
            landed(yr.at[cc, g], brecv.at[cc, g, pl.ds(0, 2 * (SLOTS - 1))])

        @pl.loop(0, 2)
        def _(u):
            l = jnp.where(s < SLOTS // 2, u, 1 - u)

            @pl.loop(0, NC // 2)
            def _(n):
                pair = [yzrecv[cc, u, 2 * n + m].reshape(512, LANES) for m in range(2)]
                value = jnp.dot(t2[u], jnp.concatenate(pair, axis=1), preferred_element_type=jnp.float32)
                value = value.astype(jnp.bfloat16)
                for m in range(2):
                    mid[:, 2 * n + m] = value[:, 128 * m : 128 * (m + 1)].reshape(LB, 16, LANES)

            @pl.loop(0, LB // 4)
            def _(n):
                spectra = []
                for e in range(4):
                    f1 = 4 * n + e
                    spectra.append(
                        jnp.dot(t3[u, f1], mid[f1].reshape(128, LANES), preferred_element_type=jnp.float32)
                    )
                outs = []
                for e in range(4):
                    f1 = 4 * n + e
                    xr_, xi_ = spectra[e][:64], spectra[e][64:]
                    hr = filt[cc, 0, l, f1].astype(jnp.float32)
                    hi = filt[cc, 1, l, f1].astype(jnp.float32)
                    outs.append(
                        jnp.concatenate([hr * xr_ - hi * xi_, hr * xi_ + hi * xr_], axis=0).astype(jnp.bfloat16)
                    )
                for e in range(4):
                    f1 = 4 * n + e
                    value = jnp.dot(t3t[u, f1], outs[e], preferred_element_type=jnp.float32)
                    mid2[f1] = value.astype(jnp.bfloat16).reshape(NC, 16, LANES)

            @pl.loop(0, NC // 2)
            def _(n):
                pair = [mid2[:, 2 * n + m].reshape(512, LANES) for m in range(2)]
                value = jnp.dot(t2t[u], jnp.concatenate(pair, axis=1), preferred_element_type=jnp.float32)
                value = value.astype(jnp.bfloat16)
                for m in range(2):
                    bsend[cc, u, 2 * n + m] = value[:, 128 * m : 128 * (m + 1)].reshape(NB, NG, 32, LANES)

        @pl.loop(0, NG)
        def _(g):
            for d in range(1, SLOTS):
                b_copy(d, cc, g).start()

            brecv[cc, g, pl.ds(place, 2)] = bsend[cc, :, c, b, g]

    def c_copy(d, cc, g):
        to = lax.rem(a + d, NA)
        return pltpu.make_async_remote_copy(
            src_ref=csend.at[cc, g, to], dst_ref=crecv.at[cc, g, a],
            send_sem=ss.at[3], recv_sem=cr.at[cc, g],
            device_id=x_device(d), device_id_type=MESH,
        )

    landed(lsem.at[16], skip)
    landed(lsem.at[17], wout)

    @pl.loop(0, CHUNKS)
    def _(n):
        cc, g = n // NG, lax.rem(n, NG)

        landed(br.at[cc, g], brecv.at[cc, g, pl.ds(0, 2 * (SLOTS - 1))])
        low = brecv[cc, g, pl.ds(0, 32)].reshape(1024, LANES)
        high = brecv[cc, g, pl.ds(32, 32)].reshape(1024, LANES)
        value = jnp.dot(mlo[...], low, preferred_element_type=jnp.float32)
        value += jnp.dot(mhi[...], high, preferred_element_type=jnp.float32)
        csend[cc, g] = value.astype(jnp.bfloat16).reshape(NA, ROWS, LANES)
        for d in (2, 1, 3):
            c_copy(d, cc, g).start()
        crecv[cc, g, a] = csend[cc, g, a]

    for g in range(NG):
        for cc in range(NCC):
            landed(cr.at[cc, g], crecv.at[cc, g, pl.ds(0, NA - 1)])
        for q in range(NA):
            for cc in range(NCC):
                at = pl.ds(256 * q + 128 * cc, 128)
                conv = crecv[cc, g, q].astype(jnp.float32)
                plus = conv + skip[:, at] * mixed[q, cc, g].astype(jnp.float32)
                gated[:, at] = (gate[g, :, at].astype(jnp.float32) * plus).astype(jnp.bfloat16)
        value = jnp.dot(gated[...], wout[...], preferred_element_type=jnp.float32)
        outv[:, 16 * g : 16 * (g + 1), :] = value.astype(jnp.bfloat16).reshape(16, 16, D)

    for cc in range(NCC):
        for g in range(NG):
            landed(ss.at[0], xrecv.at[cc, g, pl.ds(0, NA - 1)])
            landed(ss.at[1], brecv.at[cc, g, pl.ds(0, 2 * (SLOTS - 1))])
            landed(ss.at[2], brecv.at[cc, g, pl.ds(0, 2 * (SLOTS - 1))])
            landed(ss.at[3], crecv.at[cc, g, pl.ds(0, NA - 1)])


def local(tokens, norm_gain, in_weight, skip_gain, spectrum_filter, out_weight):
    tables = [jnp.asarray(t) for t in static_tables()]
    bf, f32 = jnp.bfloat16, jnp.float32
    vmem = pltpu.VMEM
    dma = pltpu.SemaphoreType.DMA
    scratch = [
        vmem((NG, 16, 16, D), bf), vmem((1, D), f32), vmem((NCC, NA, D, 256), bf), vmem((D, D), bf),
        vmem((1, D), f32), vmem((NCC, 2, 2, LB, LC, LANES), bf), vmem((D, D), bf),
        *[vmem(t.shape, f32) for t in tables],
        vmem((NA, NCC, NG, ROWS, LANES), bf),
        vmem((NG, ROWS, D), bf),
        vmem((NCC, NG, NA, ROWS, LANES), bf),
        vmem((NCC, NG, HALF, 32, LANES), bf),
        vmem((NCC, 2, NC, NB, NG, 32, LANES), bf),
        vmem((LB, NC, 16, LANES), bf),
        vmem((LB, NC, 16, LANES), bf),
        vmem((NCC, 2, NC, NB, NG, 32, LANES), bf),
        vmem((NCC, NG, 64, 32, LANES), bf),
        vmem((NCC, NG, NA, ROWS, LANES), bf),
        vmem((NCC, NG, NA, ROWS, LANES), bf),
        vmem((ROWS, D), bf),
        vmem((HALF * 32, 1024), bf), vmem((1024, 1024), bf), vmem((1024, 1024), bf),
        vmem((2, 512, 512), bf), vmem((2, 512, 512), bf),
        vmem((2, LB, 128, 128), bf), vmem((2, LB, 128, 128), bf),
        dma((18,)), dma((4,)), dma((NCC, NG)), dma((NCC, NG)), dma((NCC, NG)), dma((NCC, NG)),
    ]
    out = pl.pallas_call(
        kernel,
        out_shape=jax.ShapeDtypeStruct((16, 64, D), bf),
        in_specs=[pl.BlockSpec(memory_space=pl.ANY)] * (6 + len(tables)),
        out_specs=pl.BlockSpec(memory_space=pltpu.VMEM),
        scratch_shapes=scratch,
        compiler_params=pltpu.CompilerParams(
            collective_id=0, has_side_effects=True, vmem_limit_bytes=67043328
        ),
    )(
        tokens.reshape(16, 64, D), norm_gain.reshape(1, D), in_weight, skip_gain.reshape(1, D),
        spectrum_filter, out_weight, *tables,
    )
    return out.reshape(16, 8, 8, D)


def solution(mesh):
    in_specs = (
        P("aa", "ba", "col", None),
        P(),
        P(),
        P(),
        P(None, ("ba", "col"), None, None, "aa"),
        P(),
    )
    out_specs = P("aa", "ba", "col", None)
    return jax.shard_map(local, mesh=mesh, in_specs=in_specs, out_specs=out_specs, check_vma=False)
```

```python
import math

import jax
import jax.numpy as jnp
import numpy as np
from jax import lax
from jax.experimental import pallas as pl
from jax.experimental.pallas import tpu as pltpu
from jax.sharding import PartitionSpec as P

LA = 64
LB = 32
LC = 64
D = 1024
POINTS = LA * LB * LC
EPSILON = 1e-06
MESH = pl.DeviceIdType.MESH

NA, NB, NC = 4, 4, 8
SLOTS = NB * NC
NG = 4
NCC = 2
CHUNKS = NCC * NG
ROWS = 256
LANES = 128
HALF = LA // 2 + 1


def rounded(values):
    return np.asarray(values, np.float32).astype(jnp.bfloat16).astype(np.float32)


def dft_tables(length):
    counter = np.arange(length)
    angle = 2.0 * math.pi / length * (counter[:, None] * counter[None, :] % length)
    factor = 1.0 / math.sqrt(length)
    return rounded(np.cos(angle) * factor), rounded(np.sin(angle) * factor)


def static_tables():
    cos_a, sin_a = dft_tables(LA)
    small = np.zeros((HALF, 2, LA), np.float32)
    small[:, 0] = cos_a[:HALF]
    small[:, 1] = -sin_a[:HALF]
    small = small.reshape(HALF * 2, LA)
    table_a = np.repeat(small, 16, axis=1)
    table_lo = np.repeat(small[:LA].T, 16, axis=1)
    table_hi = np.repeat(small[2:].T, 16, axis=1)

    cos_b, sin_b = dft_tables(LB)
    lane = np.arange(512)
    j_of = 8 * (lane // 128) + 2 * (lane // 32 % 4) + lane // 8 % 2
    ri_of = lane // 16 % 2
    wc, ws = cos_b[:, j_of], sin_b[:, j_of]
    u2 = np.stack([np.where(ri_of, ws, wc), np.where(ri_of, wc, -ws)], 1).reshape(64, 512)
    v2 = np.stack([np.where(ri_of, wc, -ws), np.where(ri_of, -ws, -wc)], 1).reshape(64, 512)
    f0 = np.arange(LA)[:, None]
    sign = np.where((f0 >= LA // 2) & (ri_of[None] == 1), -1.0, 1.0)
    angle = 2.0 * math.pi / (LA * LB) * (f0 * j_of[None] % (LA * LB))
    cj, sj = np.cos(angle) * sign, np.sin(angle) * sign

    cos_c, sin_c = dft_tables(LC)
    lane = np.arange(128)
    k_of = 8 * (lane // 16) + lane % 8
    ri_of = lane // 8 % 2
    wc, ws = cos_c[:, k_of], sin_c[:, k_of]
    u3 = np.concatenate([np.where(ri_of, ws, wc), np.where(ri_of, wc, -ws)], 0)
    v3 = np.concatenate([np.where(ri_of, wc, -ws), np.where(ri_of, -ws, -wc)], 0)
    angle = 2.0 * math.pi / POINTS * (f0 * k_of[None] % POINTS)
    ca, sa = np.cos(angle), np.sin(angle)
    f1 = np.arange(LB)[:, None]
    angle = 2.0 * math.pi / (LB * LC) * (f1 * k_of[None] % (LB * LC))
    cb, sb = np.cos(angle), np.sin(angle)
    tables = (
        table_a, np.stack([table_lo, table_hi]), np.stack([u2, v2, cj, sj]),
        np.stack([u3, v3]), np.stack([ca, sa]), np.stack([cb, sb]),
    )
    return tuple(np.asarray(t, np.float32) for t in tables)


def kernel(
    tok_hbm, gain_hbm, win_hbm, skip_hbm, filt_hbm, wout_hbm,
    ta_hbm, tinv_hbm, two_hbm, three_hbm, tca_hbm, tcb_hbm,
    outv,
    tok, gain, wmix, wgate, skip, filt, wout,
    ta, tinv, two, three, tca, tcb,
    mixed, gate, xrecv, first, yzrecv, mid, mid2, bsend, brecv, csend, crecv, gated,
    m1, mlo, mhi, t2, t2t, t3, t3t,
    lsem, ss, xr, yr, br, cr,
):
    a = lax.axis_index("aa")
    b = lax.axis_index("ba")
    c = lax.axis_index("col")
    s = b * NC + c

    def fetch(n, src, dst):
        pltpu.make_async_copy(src, dst, lsem.at[n]).start()

    def landed(sem, ref):
        pltpu.make_async_copy(ref, ref, sem).wait()

    def fetch_mix(cc):
        for q in range(NA):
            for half, base in enumerate((0, 2 * D)):
                at = pl.ds(base + 256 * q + 128 * cc, 128)
                fetch(5 + cc, win_hbm.at[:, at], wmix.at[cc, q, :, pl.ds(128 * half, 128)])

    fetch(0, gain_hbm, gain)
    fetch(1, tok_hbm.at[:, pl.ds(0, 16), :], tok.at[0])
    fetch_mix(0)
    fetch(7, ta_hbm, ta)

    def fetch_rest():
        for g in range(1, NG):
            fetch(1 + g, tok_hbm.at[:, pl.ds(16 * g, 16), :], tok.at[g])
        fetch_mix(1)
        fetch(9, win_hbm.at[:, pl.ds(D, D)], wgate)
        fetch(8, tinv_hbm, tinv)
        fetch(10, two_hbm, two)
        fetch(11, three_hbm, three)
        fetch(12, tca_hbm, tca)
        fetch(13, tcb_hbm, tcb)
        for cc in range(NCC):
            fetch(14 + cc, filt_hbm.at[..., pl.ds(128 * cc, 128)], filt.at[cc])
        fetch(16, skip_hbm, skip)
        fetch(17, wout_hbm, wout)

    x_bits = [lax.rem(a, 2), a // 2]

    def x_index(d):
        picked = [1 - bit if d >> n & 1 else bit for n, bit in enumerate(x_bits)]
        return picked[0] + 2 * picked[1]

    def x_device(d):
        return {"aa": x_index(d), "ba": b, "col": c}

    bits = [lax.rem(c, 2), lax.rem(c // 2, 2), c // 4, lax.rem(b, 2), b // 2]

    def partner(d):
        picked = [1 - bit if d >> n & 1 else bit for n, bit in enumerate(bits)]
        return picked[3] + 2 * picked[4], picked[0] + 2 * picked[1] + 4 * picked[2]

    def yz_device(tb, tc):
        return {"aa": a, "ba": tb, "col": tc}

    barrier = pltpu.get_barrier_semaphore()
    for d in range(1, NA):
        pl.semaphore_signal(barrier, inc=1, device_id=x_device(d), device_id_type=MESH)

    for d in range(1, SLOTS):
        pl.semaphore_signal(barrier, inc=1, device_id=yz_device(*partner(d)), device_id_type=MESH)

    def x_copy(d, cc, g):
        to = x_index(d)
        return pltpu.make_async_remote_copy(
            src_ref=mixed.at[to, cc, g], dst_ref=xrecv.at[cc, g, a],
            send_sem=ss.at[0], recv_sem=xr.at[cc, g],
            device_id=x_device(d), device_id_type=MESH,
        )

    def mix(cc, g):
        rows = tok[g].reshape(ROWS, D)
        for q in range(NA):
            both = jnp.dot(rows, wmix[cc, q], preferred_element_type=jnp.float32)
            mixed[q, cc, g] = (both[:, :128] * both[:, 128:]).astype(jnp.bfloat16)

    def mix_send(cc, g):
        for d in (2, 1, 3):
            x_copy(d, cc, g).start()
        xrecv[cc, g, a] = mixed[a, cc, g]

    landed(lsem.at[0], gain)
    for g in range(NG):
        landed(lsem.at[1 + g], tok.at[g])

        @pl.loop(0, 4)
        def _(part):
            view = tok.at[g, pl.ds(4 * part, 4)]
            block = view[...].astype(jnp.float32).reshape(64, D)
            scale = lax.rsqrt(jnp.mean(block * block, axis=-1, keepdims=True) + EPSILON)
            view[...] = (block * scale * gain[...]).astype(jnp.bfloat16).reshape(4, 16, D)

        if g == 0:
            landed(lsem.at[5], wmix.at[0])
        if g == 0:
            fetch_rest()
        mix(0, g)
        if g == 0:
            pl.semaphore_wait(barrier, NA - 1 + SLOTS - 1)
        mix_send(0, g)

    landed(lsem.at[7], ta)
    lane16 = lax.broadcasted_iota(jnp.int32, (16, 1024), 1)
    sub16 = lax.broadcasted_iota(jnp.int32, (16, 1024), 0)
    on16 = lax.rem(lane16, 16) == sub16

    @pl.loop(0, 2 * HALF)
    def _(r):
        m1[pl.ds(pl.multiple_of(16 * r, 16), 16), :] = jnp.where(on16, ta[pl.ds(r, 1), :], 0.0).astype(jnp.bfloat16)

    landed(lsem.at[6], wmix.at[1])

    def y_copy(d, cc, g):
        tb, tc = partner(d)
        t = tb * NC + tc
        p0 = jnp.where(t < SLOTS // 2, 2 * t, LA - 1 - 2 * t)
        return pltpu.make_async_remote_copy(
            src_ref=first.at[cc, g, pl.ds(p0, 2)], dst_ref=yzrecv.at[cc, :, c, b, g],
            send_sem=ss.at[1], recv_sem=yr.at[cc, g],
            device_id=yz_device(tb, tc), device_id_type=MESH,
        )

    own0 = jnp.where(s < SLOTS // 2, 2 * s, LA - 1 - 2 * s)

    @pl.loop(0, CHUNKS)
    def _(n):
        cc, g = n // NG, lax.rem(n, NG)
        landed(xr.at[cc, g], xrecv.at[cc, g, pl.ds(0, NA - 1)])
        value = jnp.dot(m1[...], xrecv[cc, g].reshape(1024, LANES), preferred_element_type=jnp.float32)
        first[cc, g] = value.astype(jnp.bfloat16).reshape(HALF, 32, LANES)

        for d in range(1, SLOTS):
            y_copy(d, cc, g).start()

        yzrecv[cc, :, c, b, g] = first[cc, g, pl.ds(own0, 2)]

        @pl.when(n < NG)
        def _():
            mix(1, n)
            mix_send(1, n)

    landed(lsem.at[9], wgate)

    @pl.loop(0, NG)
    def _(g):
        value = jnp.dot(tok[g].reshape(ROWS, D), wgate[...], preferred_element_type=jnp.float32)
        gate[g] = value.astype(jnp.bfloat16)

    landed(lsem.at[10], two)
    landed(lsem.at[11], three)
    landed(lsem.at[12], tca)
    landed(lsem.at[13], tcb)
    for cc in range(NCC):
        landed(lsem.at[14 + cc], filt.at[cc])
    landed(lsem.at[8], tinv)

    @pl.loop(0, LA)
    def _(r):
        at = pl.ds(pl.multiple_of(16 * r, 16), 16)
        mlo[at, :] = jnp.where(on16, tinv[0, pl.ds(r, 1), :], 0.0).astype(jnp.bfloat16)
        mhi[at, :] = jnp.where(on16, tinv[1, pl.ds(r, 1), :], 0.0).astype(jnp.bfloat16)

    lane8 = lax.broadcasted_iota(jnp.int32, (16, 512), 1)
    sub8 = lax.broadcasted_iota(jnp.int32, (16, 512), 0)
    on8 = lax.rem(lane8, 8) == lax.rem(sub8, 8)
    for u in range(2):
        f0 = jnp.where(s < SLOTS // 2, 2 * s + u, 2 * s + 1 - u)
        at0 = pl.ds(f0, 1)

        @pl.loop(0, LB)
        def _(f1):
            row0, row1 = pl.ds(2 * f1, 1), pl.ds(2 * f1 + 1, 1)
            up = two[0, row0, :] * two[2, at0, :] + two[1, row0, :] * two[3, at0, :]
            low = two[0, row1, :] * two[2, at0, :] + two[1, row1, :] * two[3, at0, :]
            value = jnp.where(on8, jnp.where(sub8 < 8, up, low), 0.0)
            t2[u, pl.ds(pl.multiple_of(16 * f1, 16), 16), :] = value.astype(jnp.bfloat16)

        @pl.loop(0, 4)
        def _(r):
            at = pl.ds(pl.multiple_of(128 * r, 128), 128)
            t2t[u, :, at] = jnp.transpose(t2[u, at, :].astype(jnp.float32)).astype(jnp.bfloat16)

        @pl.loop(0, LB)
        def _(f1):
            row = pl.ds(f1, 1)
            ec = tca[0, at0, :] * tcb[0, row, :] - tca[1, at0, :] * tcb[1, row, :]
            es = tca[1, at0, :] * tcb[0, row, :] + tca[0, at0, :] * tcb[1, row, :]
            value = three[0] * ec + three[1] * es
            t3[u, f1] = value.astype(jnp.bfloat16)
            t3t[u, f1] = jnp.transpose(value).astype(jnp.bfloat16)

    place = jnp.where(s < SLOTS // 2, 2 * s, 32 + 2 * (SLOTS - 1 - s))

    def b_copy(d, cc, g):
        tb, tc = partner(d)
        return pltpu.make_async_remote_copy(
            src_ref=bsend.at[cc, :, tc, tb, g], dst_ref=brecv.at[cc, g, pl.ds(place, 2)],
            send_sem=ss.at[2], recv_sem=br.at[cc, g],
            device_id=yz_device(tb, tc), device_id_type=MESH,
        )


    @pl.loop(0, NCC)
    def _(cc):
        for g in range(NG):
            landed(yr.at[cc, g], brecv.at[cc, g, pl.ds(0, 2 * (SLOTS - 1))])

        @pl.loop(0, 2)
        def _(u):
            l = jnp.where(s < SLOTS // 2, u, 1 - u)

            @pl.loop(0, NC // 2)
            def _(n):
                pair = [yzrecv[cc, u, 2 * n + m].reshape(512, LANES) for m in range(2)]
                value = jnp.dot(t2[u], jnp.concatenate(pair, axis=1), preferred_element_type=jnp.float32)
                value = value.astype(jnp.bfloat16)
                for m in range(2):
                    mid[:, 2 * n + m] = value[:, 128 * m : 128 * (m + 1)].reshape(LB, 16, LANES)

            @pl.loop(0, LB // 4)
            def _(n):
                spectra = []
                for e in range(4):
                    f1 = 4 * n + e
                    spectra.append(
                        jnp.dot(t3[u, f1], mid[f1].reshape(128, LANES), preferred_element_type=jnp.float32)
                    )
                outs = []
                for e in range(4):
                    f1 = 4 * n + e
                    xr_, xi_ = spectra[e][:64], spectra[e][64:]
                    hr = filt[cc, 0, l, f1].astype(jnp.float32)
                    hi = filt[cc, 1, l, f1].astype(jnp.float32)
                    outs.append(
                        jnp.concatenate([hr * xr_ - hi * xi_, hr * xi_ + hi * xr_], axis=0).astype(jnp.bfloat16)
                    )
                for e in range(4):
                    f1 = 4 * n + e
                    value = jnp.dot(t3t[u, f1], outs[e], preferred_element_type=jnp.float32)
                    mid2[f1] = value.astype(jnp.bfloat16).reshape(NC, 16, LANES)

            @pl.loop(0, NC // 2)
            def _(n):
                pair = [mid2[:, 2 * n + m].reshape(512, LANES) for m in range(2)]
                value = jnp.dot(t2t[u], jnp.concatenate(pair, axis=1), preferred_element_type=jnp.float32)
                value = value.astype(jnp.bfloat16)
                for m in range(2):
                    bsend[cc, u, 2 * n + m] = value[:, 128 * m : 128 * (m + 1)].reshape(NB, NG, 32, LANES)

        @pl.loop(0, NG)
        def _(g):
            for d in range(1, SLOTS):
                b_copy(d, cc, g).start()

            brecv[cc, g, pl.ds(place, 2)] = bsend[cc, :, c, b, g]

    def c_copy(d, cc, g):
        to = x_index(d)
        return pltpu.make_async_remote_copy(
            src_ref=csend.at[cc, g, to], dst_ref=crecv.at[cc, g, a],
            send_sem=ss.at[3], recv_sem=cr.at[cc, g],
            device_id=x_device(d), device_id_type=MESH,
        )

    landed(lsem.at[16], skip)
    landed(lsem.at[17], wout)

    @pl.loop(0, CHUNKS)
    def _(n):
        cc, g = n // NG, lax.rem(n, NG)

        landed(br.at[cc, g], brecv.at[cc, g, pl.ds(0, 2 * (SLOTS - 1))])
        low = brecv[cc, g, pl.ds(0, 32)].reshape(1024, LANES)
        high = brecv[cc, g, pl.ds(32, 32)].reshape(1024, LANES)
        value = jnp.dot(mlo[...], low, preferred_element_type=jnp.float32)
        value += jnp.dot(mhi[...], high, preferred_element_type=jnp.float32)
        csend[cc, g] = value.astype(jnp.bfloat16).reshape(NA, ROWS, LANES)
        for d in (2, 1, 3):
            c_copy(d, cc, g).start()
        crecv[cc, g, a] = csend[cc, g, a]

    for g in range(NG):
        for cc in range(NCC):
            landed(cr.at[cc, g], crecv.at[cc, g, pl.ds(0, NA - 1)])
        for q in range(NA):
            for cc in range(NCC):
                at = pl.ds(256 * q + 128 * cc, 128)
                conv = crecv[cc, g, q].astype(jnp.float32)
                plus = conv + skip[:, at] * mixed[q, cc, g].astype(jnp.float32)
                gated[:, at] = (gate[g, :, at].astype(jnp.float32) * plus).astype(jnp.bfloat16)
        value = jnp.dot(gated[...], wout[...], preferred_element_type=jnp.float32)
        outv[:, 16 * g : 16 * (g + 1), :] = value.astype(jnp.bfloat16).reshape(16, 16, D)

    for cc in range(NCC):
        for g in range(NG):
            landed(ss.at[0], xrecv.at[cc, g, pl.ds(0, NA - 1)])
            landed(ss.at[1], brecv.at[cc, g, pl.ds(0, 2 * (SLOTS - 1))])
            landed(ss.at[2], brecv.at[cc, g, pl.ds(0, 2 * (SLOTS - 1))])
            landed(ss.at[3], crecv.at[cc, g, pl.ds(0, NA - 1)])


def local(tokens, norm_gain, in_weight, skip_gain, spectrum_filter, out_weight):
    tables = [jnp.asarray(t) for t in static_tables()]
    bf, f32 = jnp.bfloat16, jnp.float32
    vmem = pltpu.VMEM
    dma = pltpu.SemaphoreType.DMA
    scratch = [
        vmem((NG, 16, 16, D), bf), vmem((1, D), f32), vmem((NCC, NA, D, 256), bf), vmem((D, D), bf),
        vmem((1, D), f32), vmem((NCC, 2, 2, LB, LC, LANES), bf), vmem((D, D), bf),
        *[vmem(t.shape, f32) for t in tables],
        vmem((NA, NCC, NG, ROWS, LANES), bf),
        vmem((NG, ROWS, D), bf),
        vmem((NCC, NG, NA, ROWS, LANES), bf),
        vmem((NCC, NG, HALF, 32, LANES), bf),
        vmem((NCC, 2, NC, NB, NG, 32, LANES), bf),
        vmem((LB, NC, 16, LANES), bf),
        vmem((LB, NC, 16, LANES), bf),
        vmem((NCC, 2, NC, NB, NG, 32, LANES), bf),
        vmem((NCC, NG, 64, 32, LANES), bf),
        vmem((NCC, NG, NA, ROWS, LANES), bf),
        vmem((NCC, NG, NA, ROWS, LANES), bf),
        vmem((ROWS, D), bf),
        vmem((HALF * 32, 1024), bf), vmem((1024, 1024), bf), vmem((1024, 1024), bf),
        vmem((2, 512, 512), bf), vmem((2, 512, 512), bf),
        vmem((2, LB, 128, 128), bf), vmem((2, LB, 128, 128), bf),
        dma((18,)), dma((4,)), dma((NCC, NG)), dma((NCC, NG)), dma((NCC, NG)), dma((NCC, NG)),
    ]
    out = pl.pallas_call(
        kernel,
        out_shape=pltpu.VMEM((16, 64, D), bf),
        in_specs=[pl.BlockSpec(memory_space=pltpu.HBM)] * (6 + len(tables)),
        out_specs=pl.BlockSpec(memory_space=pltpu.VMEM),
        scratch_shapes=scratch,
        compiler_params=pltpu.CompilerParams(
            collective_id=0, has_side_effects=True, vmem_limit_bytes=58*2**20
        ),
    )(
        tokens.reshape(16, 64, D), norm_gain.reshape(1, D), in_weight, skip_gain.reshape(1, D),
        spectrum_filter, out_weight, *tables,
    )
    return out.reshape(16, 8, 8, D)


def solution(mesh):
    in_specs = (
        P("aa", "ba", "col", None),
        P(),
        P(),
        P(),
        P(None, ("ba", "col"), None, None, "aa"),
        P(),
    )
    out_specs = P("aa", "ba", "col", None)
    return jax.shard_map(local, mesh=mesh, in_specs=in_specs, out_specs=out_specs, check_vma=False)
```
